32 devices in a mesh: ma: 8 (over y, x, core), lev: 4 (over z).
Axes of the slice: x: 2, y: 2, z: 4, core: 2. Of those that a mesh axis runs over, the one named last changes fastest.
Arguments:
- spectral_state: float32 [1280, 2, 16, 1280], P('ma', None, None, 'lev'), may hold values from -6 to 6
- forcing_noise: bfloat16 [1280, 2, 16, 1280], P('ma', None, None, 'lev'), may hold values from -6 to 6
- decay_rate: float32 [16], replicated, may hold values from 0.3 to 0.95
- amplitude: float32 [1280], P('lev'), may hold values from 0.2 to 2
- legendre: bfloat16 [1280, 1280, 640], P('ma', 'lev'), may hold values from -0.0048828125 to 0.0048828125
- wave_of_slot: int32 [1280], replicated, may hold values from 0 to 1279, each once
- lat_of_row: int32 [1280], replicated, may hold values from 0 to 1279, each once
Outputs:
- new_state: float32 [1280, 2, 16, 1280], P('ma', None, None, 'lev')
- pattern: bfloat16 [16, 1280, 2560], P('lev', 'ma')
The draws below stay inside these ranges and needn't reach their ends.
Inputs may be any that keep to these rules, and one draw needn't show every extreme that they name: `wave_of_slot`: each zonal wavenumber is held by exactly one slot. `lat_of_row`: each latitude is held by exactly one row.
All inputs are finite; a program needn't handle non-finite values.
Results may differ from the reference program's by a relative error of at most 0.014.
Values may be sent and summed in bfloat16 or wider, within the bound.
A program may use at most 192 MiB of HBM per device.

```python
import math
import jax
import jax.numpy as jnp
from jax import lax

M = 1280
N = 1280
NLAT = 1280
NLON = 2560
LEVELS = 16
N_LEV = 4


def levels(own_key, dims, pieces, smallest, top_value):
    level = 1.0
    for axis_at, parts in pieces:
        draws = jax.random.uniform(jax.random.fold_in(jax.random.fold_in(own_key, 6), axis_at), (parts,), jnp.float32, smallest / len(pieces), top_value / len(pieces))
        level = level * jnp.repeat(jnp.exp(draws), dims[axis_at] // parts).reshape((-1,) + (1,) * (len(dims) - 1 - axis_at))
    return level


def normal_values(stream_key, shape, spread, most, cuts=(), kind=jnp.bfloat16):
    array = spread * jax.random.normal(stream_key, shape, jnp.float32)
    if cuts:
        array = array * levels(stream_key, shape, cuts, -0.22, 0.18)
    return jnp.clip(array, -most, most).astype(kind)


def setup_inputs(seed: int = 0) -> dict:
    key_list = jax.random.split(jax.random.key(seed), 8)
    return {
        "spectral_state": normal_values(key_list[0], (M, 2, LEVELS, N), 1.0, 6.0, ((0, 8), (3, 4)), jnp.float32),
        "forcing_noise": normal_values(key_list[1], (M, 2, LEVELS, N), 1.0, 6.0, ((0, 8), (3, 4))),
        "decay_rate": jnp.clip(jnp.exp(jax.random.uniform(key_list[2], (LEVELS,), jnp.float32, math.log(0.3), math.log(0.95))), 0.3, 0.95),
        "amplitude": jnp.clip(jnp.exp(math.log(2.0) - 2.3025851 * jax.random.uniform(key_list[3], (N,), jnp.float32) ** levels(key_list[3], (N,), ((0, 4),), -0.2, 0.2)), 0.2, 2.0),
        "legendre": normal_values(key_list[4], (M, N, NLAT // 2), (N * M) ** -0.5, 0.0048828125, ((0, 8), (1, 4))),
        "wave_of_slot": jax.random.permutation(key_list[5], M).astype(jnp.int32),
        "lat_of_row": jax.random.permutation(key_list[6], NLAT).astype(jnp.int32),
    }


def build_table(wavenum, width):
    column = jnp.arange(width, dtype=jnp.int32)
    product = (wavenum[:, None] * column[None, :]) % width
    phase_angle = product.astype(jnp.float32) * jnp.float32(2.0 * math.pi / width)
    factor = jnp.where(wavenum == 0, jnp.float32(1.0), jnp.float32(2.0))[:, None]
    stacked = jnp.stack([factor * jnp.cos(phase_angle), -factor * jnp.sin(phase_angle)], axis=1)
    return stacked.astype(jnp.bfloat16)


def reference(spectral_state, forcing_noise, decay_rate, amplitude, legendre, wave_of_slot, lat_of_row):
    wavenum = wave_of_slot.astype(jnp.int32)
    total_n = jnp.arange(N, dtype=jnp.int32)
    valid_mask = total_n[None, :] >= wavenum[:, None]
    updated = decay_rate[None, None, :, None] * spectral_state + amplitude[None, None, None, :] * forcing_noise.astype(jnp.float32)
    new_state = jnp.where(valid_mask[:, None, None, :], updated, jnp.float32(0.0))
    spectral = new_state.astype(jnp.bfloat16)
    odd_mask = ((total_n[None, :] - wavenum[:, None]) % 2) == 1
    block_len = N // N_LEV
    running = jnp.zeros((M, 2 * LEVELS, NLAT), jnp.float32)
    for block_index in range(N_LEV):
        lower = block_index * block_len
        piece = spectral[:, :, :, lower:lower + block_len].reshape(M, 2 * LEVELS, block_len)
        odd_block = odd_mask[:, None, lower:lower + block_len]
        even_part = jnp.where(odd_block, jnp.zeros_like(piece), piece)
        odd_part = jnp.where(odd_block, piece, jnp.zeros_like(piece))
        stacked = jnp.concatenate([even_part, odd_part], axis=1).astype(jnp.float32)
        weights = legendre[:, lower:lower + block_len, :].astype(jnp.float32)
        halves = jnp.einsum("scn,snj->scj", stacked, weights)
        even_sum = halves[:, :2 * LEVELS]
        odd_sum = halves[:, 2 * LEVELS:]
        full = jnp.concatenate([even_sum + odd_sum, jnp.flip(even_sum - odd_sum, axis=2)], axis=2)
        rounded = lax.optimization_barrier(full.astype(jnp.bfloat16))
        running = running + rounded.astype(jnp.float32)
    fourier = running.reshape(M, 2, LEVELS, NLAT).astype(jnp.bfloat16)
    by_row = jnp.take(fourier, lat_of_row.astype(jnp.int32), axis=3)
    dft_table = build_table(wavenum, NLON)
    pattern = jnp.einsum("srlk,srx->lkx", by_row.astype(jnp.float32), dft_table.astype(jnp.float32))
    return new_state, pattern.astype(jnp.bfloat16)
```

```python
import functools
import math

import jax
import jax.numpy as jnp
from jax import lax
from jax.experimental import pallas as pl
from jax.experimental.pallas import tpu as pltpu
from jax.sharding import PartitionSpec as P

BATCH = 8
LAG = 1
LANES = 128
f32 = jnp.float32
bf16 = jnp.bfloat16


def row_plan(rows):
    whole = rows // LANES * LANES
    rest = rows - whole
    pad = 0
    if rest:
        pad = 16
        while pad < rest:
            pad *= 2
    return whole, rest, pad


def ring_of(lev_size):
    return lev_size + LAG + 2


def table(steps, width):
    steps = jnp.abs(steps - width * jnp.floor(steps * (1.0 / width)))
    steps = jnp.minimum(steps, width - steps)
    near = jnp.minimum(steps, width / 2 - steps)
    angle = near * (2.0 * math.pi / width)
    square = angle * angle
    value = f32(1.0 / math.factorial(12))
    for order in (10, 8, 6, 4, 2, 0):
        value = value * square + (-1.0) ** (order // 2) / math.factorial(order)
    return jnp.where(steps > width / 4, -value, value)


def kernel(dims, state, noise, legendre, decay, amplitude, waves, source, wave_rows, pattern,
           states, noises, weights, own, down, up, total, pick, gathered, outbox, inbox, turned, basis, acc,
           weight_sem, state_sem, noise_sem, down_send, up_send, down_recv, up_recv, box_send, box_recv):
    ma_size, lev_size, chunks, levels, rows, half, width, pair = dims
    me = lax.axis_index("ma")
    z = lax.axis_index("lev")
    top = lev_size - 1
    tall = BATCH * 4 * levels
    whole, rest, pad = row_plan(rows)
    columns = whole + (LANES if rest else 0)
    RING = ring_of(lev_size)
    slots = chunks * BATCH
    width_n = states.shape[-1]
    level_count = levels * lev_size
    far = LAG + jnp.maximum(z, top - z)

    def fetch(c, action):
        slot = lax.rem(c, 2)
        first = c * BATCH
        for src, dst, sem in ((legendre, weights, weight_sem), (state, states, state_sem),
                              (noise, noises, noise_sem)):
            copy = pltpu.make_async_copy(src.at[pl.ds(first, BATCH)], dst.at[slot], sem.at[slot])
            getattr(copy, action)()

    def send_down(c, g):
        slot = lax.rem(c, RING)
        return pltpu.make_async_remote_copy(
            src_ref=own.at[slot, g], dst_ref=down.at[c, g], send_sem=down_send.at[slot, g],
            recv_sem=down_recv.at[c, g], device_id={"lev": z - 1}, device_id_type=pl.DeviceIdType.MESH)

    def send_up(c, g):
        slot = lax.rem(c, RING)
        return pltpu.make_async_remote_copy(
            src_ref=own.at[slot, g], dst_ref=up.at[c, g - 1], send_sem=up_send.at[slot, g - 1],
            recv_sem=up_recv.at[c, g - 1], device_id={"lev": z + 1}, device_id_type=pl.DeviceIdType.MESH)

    def send_box(c, step):
        slot = lax.rem(c, 2)
        other = lax.rem(me + step, ma_size)
        return pltpu.make_async_remote_copy(
            src_ref=outbox.at[slot, other], dst_ref=inbox.at[c, me], send_sem=box_send.at[slot, step - 1],
            recv_sem=box_recv.at[c, step - 1], device_id={"ma": other}, device_id_type=pl.DeviceIdType.MESH)

    def recv_box(c, step):
        other = lax.rem(me + ma_size - step, ma_size)
        return pltpu.make_async_remote_copy(
            src_ref=outbox.at[0, me], dst_ref=inbox.at[c, other], send_sem=box_send.at[0, step - 1],
            recv_sem=box_recv.at[c, step - 1], device_id={"ma": other}, device_id_type=pl.DeviceIdType.MESH)

    def wait_sent(c):
        for g in range(top):
            @pl.when(g < z)
            def _():
                send_down(c, g).wait_send()
        for g in range(1, lev_size):
            @pl.when(g > z)
            def _():
                send_up(c, g).wait_send()

    def partial_sums(c):
        slot = lax.rem(c, 2)
        ring = lax.rem(c, RING)

        place = z * width_n + lax.broadcasted_iota(jnp.int32, (2 * level_count, width_n), 1)

        def one(s, carry):
            offset = place - waves[me * slots + c * BATCH + s]
            value = decay[:, 0:1] * states[slot, s].reshape(2 * level_count, width_n) + amplitude[...] * noises[
                slot, s].reshape(2 * level_count, width_n).astype(f32)
            value = jnp.where(offset >= 0, value, 0.0)
            odd = (offset[0:2 * levels] & 1) == 1
            parts = []
            for g in range(lev_size):
                even = jnp.concatenate([value[g * levels:(g + 1) * levels], value[
                    level_count + g * levels:level_count + (g + 1) * levels]], axis=0)
                parts += [even, jnp.where(odd, -even, even)]
            coef = jnp.concatenate(parts, axis=0).astype(bf16)
            product = jnp.dot(coef, weights[slot, s], preferred_element_type=f32)
            product = product.reshape(lev_size, 4 * levels, half)
            for g in range(lev_size):
                own[ring, g, pl.ds(pl.multiple_of(s * 4 * levels, 16), 4 * levels), :] = product[g].astype(bf16)
            return carry

        lax.fori_loop(0, BATCH, one, 0, unroll=4)

    def add(ring, g, arrived):
        own[ring, g] = (own[ring, g].astype(f32) + arrived.astype(f32)).astype(bf16)

    def pass_down(c):
        ring = lax.rem(c, RING)
        for g in range(top):
            @pl.when(g <= z)
            def _():
                send_down(c, g).wait_recv()

            @pl.when(g < z)
            def _():
                add(ring, g, down[c, g])
                send_down(c, g).start()

    def pass_up(c):
        ring = lax.rem(c, RING)
        for g in range(top, 0, -1):
            @pl.when(g >= z)
            def _():
                send_up(c, g).wait_recv()

            @pl.when(g > z)
            def _():
                add(ring, g, up[c, g - 1])
                send_up(c, g).start()

    def gather(c):
        total[...] = own[lax.rem(c, RING), z].astype(f32)

        @pl.when(z < top)
        def _():
            total[...] += down[c, z].astype(f32)

        @pl.when(z > 0)
        def _():
            total[...] += up[c, z - 1].astype(f32)

    def exchange(c):
        slot = lax.rem(c, 2)

        @pl.when(c >= 2)
        def _():
            for step in range(1, ma_size):
                send_box(c - 2, step).wait_send()

        parts = total[...].reshape(BATCH, 2, 2 * levels, half)
        flat = jnp.concatenate([parts[:, 0].reshape(-1, half), parts[:, 1].reshape(-1, half)], axis=1).astype(bf16)
        for step in range(ma_size):
            other = lax.rem(me + step, ma_size)
            rows_of = jnp.dot(flat, pick[other], preferred_element_type=f32)
            for t in range(columns // LANES):
                gathered[t] = rows_of[:, t * LANES:(t + 1) * LANES]

            def put(lanes, value):
                if step:
                    outbox[slot, other, :, lanes] = value.astype(bf16)
                else:
                    inbox[c, me, :, lanes] = value.astype(bf16)

            for l in range(levels):
                for t in range(whole // LANES):
                    put(pl.ds(l * whole + t * LANES, LANES), gathered[t, pl.ds(l, 2 * BATCH, stride=levels), :])
            if rest:
                each = LANES // pad
                lane = lax.broadcasted_iota(jnp.int32, (2 * BATCH, LANES), 1) // pad
                for first in range(0, levels, each):
                    mixed = None
                    for l in range(first, min(first + each, levels)):
                        value = gathered[whole // LANES, pl.ds(l, 2 * BATCH, stride=levels), :]
                        mixed = value if mixed is None else jnp.where(lane == l - first, value, mixed)
                    put(pl.ds(levels * whole + first * pad, LANES), mixed)
            if step:
                send_box(c, step).start()

    def transform(c):
        depth = ma_size * 2 * BATCH
        first = (c - (pair - 1)) * depth
        deep = pl.ds(pl.multiple_of(first, 256), pair * depth)
        wave = wave_rows[deep, :]
        lane = lax.broadcasted_iota(jnp.int32, wave.shape, 1).astype(f32)
        part = (lax.broadcasted_iota(jnp.int32, wave.shape, 0) & 1).astype(f32)
        factor = jnp.where(wave == 0.0, 1.0, 2.0)
        fine = wave * lane
        fine_cos, fine_sin = table(fine, width), table(fine - width // 4, width)
        rough = wave * (lane * LANES) + part * (width // 4)
        coarse_cos, coarse_sin = factor * table(rough, width), factor * table(rough - width // 4, width)
        blocks = width // LANES
        for a in range(blocks):
            value = coarse_cos[:, a:a + 1] * fine_cos - coarse_sin[:, a:a + 1] * fine_sin
            basis[:, a * LANES:(a + 1) * LANES] = value.astype(bf16)
        for k in range(pair):
            for step in range(1, ma_size):
                recv_box(c - (pair - 1) + k, step).wait_recv()
        spread = inbox[pl.ds(c - (pair - 1), pair)]
        turned[...] = jnp.transpose(spread.reshape(pair * depth, spread.shape[-1]))

        def one(n, carry):
            lanes = pl.ds(pl.multiple_of(n * 256, 256), 256)
            acc[:, lanes] += jnp.dot(turned[...], basis[:, lanes], preferred_element_type=f32)
            return carry

        lax.fori_loop(0, width // 256, one, 0)

    barrier = pltpu.get_barrier_semaphore()
    for step in range(1, ma_size):
        pl.semaphore_signal(barrier, inc=1, device_id={"ma": lax.rem(me + step, ma_size)},
                            device_id_type=pl.DeviceIdType.MESH)

    @pl.when(z > 0)
    def _():
        pl.semaphore_signal(barrier, inc=1, device_id={"lev": z - 1}, device_id_type=pl.DeviceIdType.MESH)

    @pl.when(z < top)
    def _():
        pl.semaphore_signal(barrier, inc=1, device_id={"lev": z + 1}, device_id_type=pl.DeviceIdType.MESH)

    fetch(0, "start")
    inner = (z > 0) & (z < top)

    @pl.when(inner)
    def _():
        pl.semaphore_wait(barrier, ma_size + 1)

    @pl.when(jnp.logical_not(inner))
    def _():
        pl.semaphore_wait(barrier, ma_size)

    def step(i, carry):
        @pl.when(i < chunks)
        def _():
            @pl.when(i + 1 < chunks)
            def _():
                fetch(i + 1, "start")

            fetch(i, "wait")

            @pl.when(i >= RING)
            def _():
                wait_sent(i - RING)

            partial_sums(i)

            @pl.when(z == top)
            def _():
                for g in range(top):
                    send_down(i, g).start()

            @pl.when(z == 0)
            def _():
                for g in range(top, 0, -1):
                    send_up(i, g).start()

        @pl.when(i == 0)
        def _():
            acc[...] = jnp.zeros_like(acc)
            row = lax.broadcasted_iota(jnp.int32, (2 * half, columns), 0)
            for j in range(ma_size):
                pick[j] = jnp.where(row == source[:, j * columns:(j + 1) * columns], 1.0, 0.0).astype(bf16)

        def stage(lag, active, work):
            c = i - lag

            @pl.when((c >= 0) & (c < chunks) & active)
            def _():
                work(c)

        stage(LAG + top - z, z < top, pass_down)
        stage(LAG + z, z > 0, pass_up)
        stage(far, z >= 0, gather)
        stage(far, z >= 0, exchange)
        stage(far + 1, lax.rem(i - far - 1 + pair, pair) == pair - 1, transform)
        return carry

    lax.fori_loop(0, chunks + LAG + top + 1, step, 0)
    for c in range(max(0, chunks - RING), chunks):
        wait_sent(c)
    for c in range(max(0, chunks - 2), chunks):
        for s in range(1, ma_size):
            send_box(c, s).wait_send()
    for l in range(levels):
        if whole:
            pattern[l, 0:whole, :] = acc[l * whole:(l + 1) * whole, :].astype(bf16)
        if rest:
            first = levels * whole + l * pad
            pattern[l, whole:rows, :] = acc[first:first + rest, :].astype(bf16)


def make_body(ma_size, lev_size):
    def body(spectral_state, forcing_noise, decay_rate, amplitude, legendre, wave_of_slot, lat_of_row):
        slot_count, _, level_count, width_n = spectral_state.shape
        levels = level_count // lev_size
        half = legendre.shape[2]
        lat_count = lat_of_row.shape[0]
        width = 2 * lat_count
        rows = lat_count // ma_size
        chunks = slot_count // BATCH
        lev = lax.axis_index("lev")
        wavenum = lax.dynamic_slice_in_dim(wave_of_slot, lax.axis_index("ma") * slot_count, slot_count)
        total_n = lev * width_n + jnp.arange(width_n, dtype=jnp.int32)
        offset = total_n[None, :] - wavenum[:, None]
        updated = decay_rate[None, None, :, None] * spectral_state + amplitude[
            None, None, None, :
        ] * forcing_noise.astype(f32)
        new_state = jnp.where((offset >= 0)[:, None, None, :], updated, f32(0.0))
        whole, rest, pad = row_plan(rows)
        source = jnp.where(lat_of_row < half, lat_of_row, half + lat_count - 1 - lat_of_row)
        source = source.astype(jnp.int32).reshape(ma_size, rows)
        if rest:
            tail = jnp.pad(source[:, whole:], ((0, 0), (0, pad - rest)), constant_values=-1)
            source = jnp.concatenate([source[:, :whole], jnp.tile(tail, (1, LANES // pad))], axis=1)
        columns = source.shape[1]
        wave_rows = wave_of_slot.astype(f32).reshape(ma_size, chunks, BATCH).transpose(1, 0, 2).reshape(-1)
        wave_rows = jnp.broadcast_to(jnp.repeat(wave_rows, 2)[:, None], (2 * wave_rows.shape[0], LANES))
        decay = jnp.broadcast_to(jnp.tile(decay_rate, 2)[:, None], (2 * level_count, LANES))
        depth = ma_size * 2 * BATCH
        pair = max(1, 256 // depth)
        spread = levels * (whole + pad)
        tall = BATCH * 4 * levels
        dims = (ma_size, lev_size, chunks, levels, rows, half, width, pair)
        any_space = pl.BlockSpec(memory_space=pl.ANY)
        vmem = pl.BlockSpec(memory_space=pltpu.VMEM)
        dma = pltpu.SemaphoreType.DMA
        pattern = pl.pallas_call(
            functools.partial(kernel, dims),
            out_shape=jax.ShapeDtypeStruct((levels, rows, width), bf16),
            in_specs=[any_space, any_space, any_space, vmem, vmem, pl.BlockSpec(memory_space=pltpu.SMEM), vmem, vmem],
            out_specs=vmem,
            scratch_shapes=[
                pltpu.VMEM((2, BATCH, 2, level_count, width_n), f32),
                pltpu.VMEM((2, BATCH, 2, level_count, width_n), bf16),
                pltpu.VMEM((2, BATCH, width_n, half), bf16),
                pltpu.VMEM((ring_of(lev_size), lev_size, tall, half), bf16),
                pltpu.VMEM((chunks, lev_size - 1, tall, half), bf16),
                pltpu.VMEM((chunks, lev_size - 1, tall, half), bf16),
                pltpu.VMEM((tall, half), f32),
                pltpu.VMEM((ma_size, 2 * half, columns), bf16),
                pltpu.VMEM((columns // LANES, BATCH * 2 * levels, LANES), f32),
                pltpu.VMEM((2, ma_size, 2 * BATCH, spread), bf16),
                pltpu.VMEM((chunks, ma_size, 2 * BATCH, spread), bf16),
                pltpu.VMEM((spread, pair * depth), bf16),
                pltpu.VMEM((pair * depth, width), bf16),
                pltpu.VMEM((spread, width), f32),
                dma((2,)), dma((2,)), dma((2,)),
                dma((ring_of(lev_size), lev_size - 1)), dma((ring_of(lev_size), lev_size - 1)),
                dma((chunks, lev_size - 1)), dma((chunks, lev_size - 1)),
                dma((2, ma_size - 1)), dma((chunks, ma_size - 1)),
            ],
            compiler_params=pltpu.CompilerParams(
                collective_id=0, has_side_effects=True, vmem_limit_bytes=64 * 1024 * 1024 - 65536),
        )(spectral_state, forcing_noise, legendre, decay, amplitude.reshape(1, -1), wave_of_slot.astype(jnp.int32),
          source.reshape(1, -1), wave_rows)
        return (new_state, pattern)

    return body


def solution(mesh):
    return jax.shard_map(
        make_body(mesh.shape["ma"], mesh.shape["lev"]),
        mesh=mesh,
        in_specs=(
            P("ma", None, None, "lev"),
            P("ma", None, None, "lev"),
            P(),
            P("lev"),
            P("ma", "lev", None),
            P(),
            P(),
        ),
        out_specs=(P("ma", None, None, "lev"), P("lev", "ma", None)),
        check_vma=False,
    )
```

```python
import functools
import math

import jax
import jax.numpy as jnp
from jax import lax
from jax.experimental import pallas as pl
from jax.experimental.pallas import tpu as pltpu
from jax.sharding import PartitionSpec as P

BATCH = 8
SPARE = 3 * 1024 * 1024
LAG = 1
LANES = 128
f32 = jnp.float32
bf16 = jnp.bfloat16


def row_plan(rows):
    whole = rows // LANES * LANES
    rest = rows - whole
    pad = 0
    if rest:
        pad = 16
        while pad < rest:
            pad *= 2
    return whole, rest, pad


def ring_of(lev_size):
    return lev_size + LAG + 2


def table(steps, width):
    steps = jnp.abs(steps - width * jnp.floor(steps * (1.0 / width)))
    steps = jnp.minimum(steps, width - steps)
    near = jnp.minimum(steps, width / 2 - steps)
    angle = near * (2.0 * math.pi / width)
    square = angle * angle
    value = f32(1.0 / math.factorial(12))
    for order in (10, 8, 6, 4, 2, 0):
        value = value * square + (-1.0) ** (order // 2) / math.factorial(order)
    return jnp.where(steps > width / 4, -value, value)


def kernel(dims, state, noise, legendre, decay_in, amplitude_in, waves_in, source_in, new_state, pattern,
           decay, amplitude, waves, source, states, noises, fresh, weights, decays, wave_rows, own, arrived, total, pick, gathered, outbox, inbox, turned, basis, acc,
           small_sem, weight_sem, state_sem, noise_sem, fresh_sem, down_send, up_send, down_recv, up_recv, box_send, box_recv):
    ma_size, lev_size, chunks, levels, rows, half, width, pair = dims
    me = lax.axis_index("ma")
    z = lax.axis_index("lev")
    top = lev_size - 1
    tall = BATCH * 4 * levels
    whole, rest, pad = row_plan(rows)
    columns = whole + (LANES if rest else 0)
    RING = ring_of(lev_size)
    slots = chunks * BATCH
    width_n = states.shape[-1]
    level_count = levels * lev_size
    far = LAG + jnp.maximum(z, top - z)

    def fetch(c, action):
        slot = lax.rem(c, 2)
        first = c * BATCH
        for src, dst, sem in ((state, states, state_sem), (noise, noises, noise_sem),
                              (legendre, weights, weight_sem)):
            copy = pltpu.make_async_copy(src.at[pl.ds(first, BATCH)], dst.at[slot], sem.at[slot])
            getattr(copy, action)()

    def store_fresh(c):
        slot = lax.rem(c, 2)
        return pltpu.make_async_copy(fresh.at[slot], new_state.at[pl.ds(c * BATCH, BATCH)], fresh_sem.at[slot])

    def send_down(c, g):
        slot = lax.rem(c, RING)
        return pltpu.make_async_remote_copy(
            src_ref=own.at[slot, g], dst_ref=arrived.at[c, g], send_sem=down_send.at[slot, g],
            recv_sem=down_recv.at[c, g], device_id={"lev": z - 1}, device_id_type=pl.DeviceIdType.MESH)

    def send_up(c, g):
        slot = lax.rem(c, RING)
        return pltpu.make_async_remote_copy(
            src_ref=own.at[slot, g], dst_ref=arrived.at[c, g + 1], send_sem=up_send.at[slot, g - 1],
            recv_sem=up_recv.at[c, g - 1], device_id={"lev": z + 1}, device_id_type=pl.DeviceIdType.MESH)

    def send_box(c, step):
        slot = lax.rem(c, 2)
        other = lax.rem(me + step, ma_size)
        return pltpu.make_async_remote_copy(
            src_ref=outbox.at[slot, other], dst_ref=inbox.at[c, me], send_sem=box_send.at[slot, step - 1],
            recv_sem=box_recv.at[c, step - 1], device_id={"ma": other}, device_id_type=pl.DeviceIdType.MESH)

    def recv_box(c, step):
        other = lax.rem(me + ma_size - step, ma_size)
        return pltpu.make_async_remote_copy(
            src_ref=outbox.at[0, me], dst_ref=inbox.at[c, other], send_sem=box_send.at[0, step - 1],
            recv_sem=box_recv.at[c, step - 1], device_id={"ma": other}, device_id_type=pl.DeviceIdType.MESH)

    def wait_sent(c):
        for g in range(top):
            @pl.when(g < z)
            def _():
                send_down(c, g).wait_send()
        for g in range(1, lev_size):
            @pl.when(g > z)
            def _():
                send_up(c, g).wait_send()

    def partial_sums(c):
        slot = lax.rem(c, 2)
        ring = lax.rem(c, RING)

        place = z * width_n + lax.broadcasted_iota(jnp.int32, (2 * level_count, width_n), 1)

        @pl.when(c >= 2)
        def _():
            store_fresh(c - 2).wait()

        def one(s, carry):
            offset = place - waves[me * slots + c * BATCH + s]
            value = decays[:, 0:1] * states[slot, s].reshape(2 * level_count, width_n) + amplitude[...] * noises[
                slot, s].reshape(2 * level_count, width_n).astype(f32)
            value = jnp.where(offset >= 0, value, 0.0)
            fresh[slot, s] = value.reshape(2, level_count, width_n)
            odd = (offset[0:2 * levels] & 1) == 1
            parts = []
            for g in range(lev_size):
                even = jnp.concatenate([value[g * levels:(g + 1) * levels], value[
                    level_count + g * levels:level_count + (g + 1) * levels]], axis=0)
                parts += [even, jnp.where(odd, -even, even)]
            coef = jnp.concatenate(parts, axis=0).astype(bf16)
            product = jnp.dot(coef, weights[slot, s], preferred_element_type=f32)
            product = product.reshape(lev_size, 4 * levels, half)
            for g in range(lev_size):
                own[ring, g, pl.ds(pl.multiple_of(s * 4 * levels, 16), 4 * levels), :] = product[g].astype(bf16)
            return carry

        lax.fori_loop(0, BATCH, one, 0, unroll=4)
        store_fresh(c).start()

    def add(ring, g, value):
        own[ring, g] = (own[ring, g].astype(f32) + value.astype(f32)).astype(bf16)

    def pass_down(c):
        ring = lax.rem(c, RING)
        for g in range(top):
            @pl.when(g < z)
            def _():
                send_down(c, g).wait_recv()
                add(ring, g, arrived[c, g])
                send_down(c, g).start()

    def pass_up(c):
        ring = lax.rem(c, RING)
        for g in range(top, 0, -1):
            @pl.when(g > z)
            def _():
                send_up(c, g).wait_recv()
                add(ring, g, arrived[c, g + 1])
                send_up(c, g).start()

    def gather(c):
        total[...] = own[lax.rem(c, RING), z].astype(f32)

        @pl.when(z < top)
        def _():
            send_down(c, z).wait_recv()
            total[...] += arrived[c, z].astype(f32)

        @pl.when(z > 0)
        def _():
            send_up(c, z).wait_recv()
            total[...] += arrived[c, z + 1].astype(f32)

    def exchange(c):
        slot = lax.rem(c, 2)

        @pl.when(c >= 2)
        def _():
            for step in range(1, ma_size):
                send_box(c - 2, step).wait_send()

        parts = total[...].reshape(BATCH, 2, 2 * levels, half)
        flat = jnp.concatenate([parts[:, 0].reshape(-1, half), parts[:, 1].reshape(-1, half)], axis=1).astype(bf16)
        for first in range(0, ma_size * columns, 1024):
            rows_of = jnp.dot(flat, pick[:, first:first + 1024], preferred_element_type=f32)
            for t in range(1024 // LANES):
                gathered[first // LANES + t] = rows_of[:, t * LANES:(t + 1) * LANES]
        for step in range(ma_size):
            other = lax.rem(me + step, ma_size)
            tile = other * (columns // LANES)

            def put(lanes, value):
                if step:
                    outbox[slot, other, :, lanes] = value.astype(bf16)
                else:
                    inbox[c, me, :, lanes] = value.astype(bf16)

            for l in range(levels):
                for t in range(whole // LANES):
                    put(pl.ds(l * whole + t * LANES, LANES), gathered[tile + t, pl.ds(l, 2 * BATCH, stride=levels), :])
            if rest:
                each = LANES // pad
                lane = lax.broadcasted_iota(jnp.int32, (2 * BATCH, LANES), 1) // pad
                for first in range(0, levels, each):
                    mixed = None
                    for l in range(first, min(first + each, levels)):
                        value = gathered[tile + whole // LANES, pl.ds(l, 2 * BATCH, stride=levels), :]
                        mixed = value if mixed is None else jnp.where(lane == l - first, value, mixed)
                    put(pl.ds(levels * whole + first * pad, LANES), mixed)
            if step:
                send_box(c, step).start()

    depth = ma_size * 2 * BATCH
    held = basis.shape[0]

    def waves_of(c):
        row = lax.broadcasted_iota(jnp.int32, (2 * BATCH, LANES), 0) // 2

        def one(n, carry):
            first = lax.rem(n, ma_size) * slots + (c - (pair - 1) + n // ma_size) * BATCH
            value = jnp.zeros((2 * BATCH, LANES), f32)
            for s in range(BATCH):
                value = jnp.where(row == s, waves[first + s].astype(f32), value)
            wave_rows[pl.ds(pl.multiple_of(n * 2 * BATCH, 2 * BATCH), 2 * BATCH), :] = value
            return carry

        lax.fori_loop(0, pair * ma_size, one, 0)
        wave = wave_rows[...]
        lane = lax.broadcasted_iota(jnp.int32, wave.shape, 1).astype(f32)
        part = (lax.broadcasted_iota(jnp.int32, wave.shape, 0) & 1).astype(f32)
        factor = jnp.where(wave == 0.0, 1.0, 2.0)
        fine = wave * lane
        fine_cos, fine_sin = table(fine, width), table(fine - width // 4, width)
        rough = wave * (lane * LANES) + part * (width // 4)
        coarse_cos, coarse_sin = factor * table(rough, width), factor * table(rough - width // 4, width)
        slot = lax.rem(c // pair, held)
        for a in range(width // LANES):
            value = coarse_cos[:, a:a + 1] * fine_cos - coarse_sin[:, a:a + 1] * fine_sin
            basis[slot, :, a * LANES:(a + 1) * LANES] = value.astype(bf16)

    def turn(c):
        for k in range(pair):
            for step in range(1, ma_size):
                recv_box(c - (pair - 1) + k, step).wait_recv()
        spread = inbox[pl.ds(c - (pair - 1), pair)]
        turned[...] = jnp.transpose(spread.reshape(pair * depth, spread.shape[-1]))

    def transform(c):
        turn(c)

        def one(n, carry):
            lanes = pl.ds(pl.multiple_of(n * 256, 256), 256)
            acc[:, lanes] += jnp.dot(turned[...], basis[lax.rem(c // pair, held), :, lanes], preferred_element_type=f32)
            return carry

        lax.fori_loop(0, width // 256, one, 0)

    def finish(c):
        turn(c)
        for n in range(width // 256):
            lanes = pl.ds(n * 256, 256)
            value = (acc[:, lanes] + jnp.dot(
                turned[...], basis[(c // pair) % held, :, lanes], preferred_element_type=f32)).astype(bf16)
            for l in range(levels):
                if whole:
                    pattern[l, 0:whole, lanes] = value[l * whole:(l + 1) * whole]
                if rest:
                    first = levels * whole + l * pad
                    pattern[l, whole:rows, lanes] = value[first:first + rest]

    barrier = pltpu.get_barrier_semaphore()
    for step in range(1, ma_size):
        pl.semaphore_signal(barrier, inc=1, device_id={"ma": lax.rem(me + step, ma_size)},
                            device_id_type=pl.DeviceIdType.MESH)

    @pl.when(z > 0)
    def _():
        pl.semaphore_signal(barrier, inc=1, device_id={"lev": z - 1}, device_id_type=pl.DeviceIdType.MESH)

    @pl.when(z < top)
    def _():
        pl.semaphore_signal(barrier, inc=1, device_id={"lev": z + 1}, device_id_type=pl.DeviceIdType.MESH)

    small = [pltpu.make_async_copy(src, dst, small_sem.at[n]) for n, (src, dst) in enumerate((
        (decay_in, decay), (amplitude_in, amplitude), (waves_in, waves), (source_in, source)))]
    for copy in small:
        copy.start()
    fetch(0, "start")
    for copy in small:
        copy.wait()
    level = lax.rem(lax.broadcasted_iota(jnp.int32, decays.shape, 0), level_count)
    rate = jnp.zeros(decays.shape, f32)
    for l in range(level_count):
        rate = jnp.where(level == l, decay[l], rate)
    decays[...] = rate
    fetch(0, "wait")
    partial_sums(0)
    inner = (z > 0) & (z < top)

    @pl.when(inner)
    def _():
        pl.semaphore_wait(barrier, ma_size + 1)

    @pl.when(jnp.logical_not(inner))
    def _():
        pl.semaphore_wait(barrier, ma_size)

    def step(i, carry):
        @pl.when(i < chunks)
        def _():
            @pl.when(i + 1 < chunks)
            def _():
                fetch(i + 1, "start")

            @pl.when(i > 0)
            def _():
                fetch(i, "wait")

                @pl.when(i >= RING)
                def _():
                    wait_sent(i - RING)

                partial_sums(i)

            @pl.when(z == top)
            def _():
                for g in range(top - 1):
                    send_down(i, g).start()

                @pl.when(i > 0)
                def _():
                    send_down(i - 1, top - 1).start()

                @pl.when(i == chunks - 1)
                def _():
                    send_down(i, top - 1).start()

            @pl.when(z == 0)
            def _():
                for g in range(top, 1, -1):
                    send_up(i, g).start()

                @pl.when(i > 0)
                def _():
                    send_up(i - 1, 1).start()

                @pl.when(i == chunks - 1)
                def _():
                    send_up(i, 1).start()

        @pl.when(i == 0)
        def _():
            acc[...] = jnp.zeros_like(acc)
            row = lax.broadcasted_iota(jnp.int32, (2 * half, columns), 0)
            for j in range(ma_size):
                pick[:, j * columns:(j + 1) * columns] = jnp.where(row == source[:, j * columns:(j + 1) * columns], 1.0, 0.0).astype(bf16)

        def stage(lag, active, work):
            c = i - lag

            @pl.when((c >= 0) & (c < chunks) & active)
            def _():
                work(c)

        early = far - 2
        stage(early, lax.rem(i - early + pair, pair) == pair - 1, waves_of)
        stage(LAG + top - z, z < top, pass_down)
        stage(LAG + z, z > 0, pass_up)
        stage(far, z >= 0, gather)
        stage(far, z >= 0, exchange)
        stage(far + 1, (lax.rem(i - far - 1 + pair, pair) == pair - 1) & (i - far - 1 < chunks - 1), transform)
        return carry

    lax.fori_loop(0, chunks + LAG + top, step, 0)
    finish(chunks - 1)
    for c in range(max(0, chunks - 2), chunks):
        store_fresh(c).wait()
    for c in range(max(0, chunks - RING), chunks):
        wait_sent(c)
    for c in range(max(0, chunks - 2), chunks):
        for s in range(1, ma_size):
            send_box(c, s).wait_send()


def make_body(ma_size, lev_size):
    def body(spectral_state, forcing_noise, decay_rate, amplitude, legendre, wave_of_slot, lat_of_row):
        slot_count, _, level_count, width_n = spectral_state.shape
        levels = level_count // lev_size
        half = legendre.shape[2]
        lat_count = lat_of_row.shape[0]
        width = 2 * lat_count
        rows = lat_count // ma_size
        chunks = slot_count // BATCH
        whole, rest, pad = row_plan(rows)
        source = jnp.where(lat_of_row < half, lat_of_row, half + lat_count - 1 - lat_of_row)
        source = source.astype(jnp.int32).reshape(ma_size, rows)
        if rest:
            tail = jnp.pad(source[:, whole:], ((0, 0), (0, pad - rest)), constant_values=-1)
            source = jnp.concatenate([source[:, :whole], jnp.tile(tail, (1, LANES // pad))], axis=1)
        columns = source.shape[1]
        depth = ma_size * 2 * BATCH
        pair = max(1, 256 // depth)
        spread = levels * (whole + pad)
        tall = BATCH * 4 * levels
        dims = (ma_size, lev_size, chunks, levels, rows, half, width, pair)
        any_space = pl.BlockSpec(memory_space=pl.ANY)
        vmem = pl.BlockSpec(memory_space=pltpu.VMEM)
        dma = pltpu.SemaphoreType.DMA
        source = source.reshape(1, -1)
        ring = ring_of(lev_size)
        arrays = [
            ((1, width_n), f32), (source.shape, jnp.int32),
            ((2, BATCH, 2, level_count, width_n), f32),
            ((2, BATCH, 2, level_count, width_n), bf16),
            ((2, BATCH, 2, level_count, width_n), f32),
            ((2, BATCH, width_n, half), bf16),
            ((2 * level_count, LANES), f32),
            ((pair * depth, LANES), f32),
            ((ring, lev_size, tall, half), bf16),
            ((chunks, lev_size + 1, tall, half), bf16),
            ((tall, half), f32),
            ((2 * half, ma_size * columns), bf16),
            ((ma_size * columns // LANES, BATCH * 2 * levels, LANES), f32),
            ((2, ma_size, 2 * BATCH, spread), bf16),
            ((chunks, ma_size, 2 * BATCH, spread), bf16),
            ((spread, pair * depth), bf16),
            ((3 // pair + 1, pair * depth, width), bf16),
            ((spread, width), f32),
        ]
        scratch = [pltpu.VMEM(shape, kind) for shape, kind in arrays]
        bytes_held = sum(math.prod(shape[:-1]) * -(-shape[-1] // LANES) * LANES * jnp.dtype(kind).itemsize
                         for shape, kind in arrays)
        smem = pltpu.SMEM
        return pl.pallas_call(
            functools.partial(kernel, dims),
            out_shape=(jax.ShapeDtypeStruct(spectral_state.shape, f32),
                       jax.ShapeDtypeStruct((levels, rows, width), bf16)),
            in_specs=[any_space, any_space, any_space] + [pl.BlockSpec(memory_space=pltpu.HBM)] * 4,
            out_specs=(any_space, vmem),
            scratch_shapes=[
                smem(decay_rate.shape, f32), scratch[0], smem(wave_of_slot.shape, jnp.int32), *scratch[1:],
                dma((4,)),
                dma((2,)), dma((2,)), dma((2,)), dma((2,)),
                dma((ring, lev_size - 1)), dma((ring, lev_size - 1)),
                dma((chunks, lev_size - 1)), dma((chunks, lev_size - 1)),
                dma((2, ma_size - 1)), dma((chunks, ma_size - 1)),
            ],
            compiler_params=pltpu.CompilerParams(
                collective_id=0, has_side_effects=True, vmem_limit_bytes=min(bytes_held + SPARE, 67043328)),
        )(spectral_state, forcing_noise, legendre, decay_rate, amplitude.reshape(1, -1), wave_of_slot.astype(jnp.int32), source)

    return body


def solution(mesh):
    return jax.shard_map(
        make_body(mesh.shape["ma"], mesh.shape["lev"]),
        mesh=mesh,
        in_specs=(
            P("ma", None, None, "lev"),
            P("ma", None, None, "lev"),
            P(),
            P("lev"),
            P("ma", "lev", None),
            P(),
            P(),
        ),
        out_specs=(P("ma", None, None, "lev"), P("lev", "ma", None)),
        check_vma=False,
    )
```

```python
import functools
import math

import jax
import jax.numpy as jnp
from jax import lax
from jax.experimental import pallas as pl
from jax.experimental.pallas import tpu as pltpu
from jax.sharding import PartitionSpec as P

BATCH = 8
PIECES = 8
SPARE = 3 * 1024 * 1024
LAG = 1
LANES = 128
f32 = jnp.float32
bf16 = jnp.bfloat16


def row_plan(rows):
    whole = rows // LANES * LANES
    rest = rows - whole
    pad = 0
    if rest:
        pad = 16
        while pad < rest:
            pad *= 2
    return whole, rest, pad


def ring_of(lev_size):
    return lev_size + LAG + 2


def table(steps, width):
    steps = jnp.abs(steps - width * jnp.floor(steps * (1.0 / width)))
    steps = jnp.minimum(steps, width - steps)
    near = jnp.minimum(steps, width / 2 - steps)
    angle = near * (2.0 * math.pi / width)
    square = angle * angle
    value = f32(1.0 / math.factorial(12))
    for order in (10, 8, 6, 4, 2, 0):
        value = value * square + (-1.0) ** (order // 2) / math.factorial(order)
    return jnp.where(steps > width / 4, -value, value)


def kernel(dims, state, noise, legendre, small_in, source_in, new_state, pattern,
           decay, amplitude, waves, source, states, noises, fresh, weights, decays, wave_rows, own, arrived, total, pick, gathered, outbox, inbox, turned, basis, acc,
           small_sem, weight_sem, state_sem, noise_sem, fresh_sem, down_send, up_send, down_recv, up_recv, box_send, box_recv):
    ma_size, lev_size, chunks, levels, rows, half, width, pair = dims
    me = lax.axis_index("ma")
    z = lax.axis_index("lev")
    top = lev_size - 1
    tall = BATCH * 4 * levels
    whole, rest, pad = row_plan(rows)
    columns = whole + (LANES if rest else 0)
    RING = ring_of(lev_size)
    slots = chunks * BATCH
    width_n = states.shape[-1]
    level_count = levels * lev_size
    far = LAG + jnp.maximum(z, top - z)

    def fetch(c, action):
        slot = lax.rem(c, 2)
        first = c * BATCH
        for src, dst, sem in ((state, states, state_sem), (noise, noises, noise_sem),
                              (legendre, weights, weight_sem)):
            copy = pltpu.make_async_copy(src.at[pl.ds(first, BATCH)], dst.at[slot], sem.at[slot])
            getattr(copy, action)()

    def store_fresh(c):
        slot = lax.rem(c, 2)
        return pltpu.make_async_copy(fresh.at[slot], new_state.at[pl.ds(c * BATCH, BATCH)], fresh_sem.at[slot])

    def send_down(c, g):
        slot = lax.rem(c, RING)
        return pltpu.make_async_remote_copy(
            src_ref=own.at[slot, g], dst_ref=arrived.at[c, g], send_sem=down_send.at[slot, g],
            recv_sem=down_recv.at[c, g], device_id={"lev": z - 1}, device_id_type=pl.DeviceIdType.MESH)

    def send_up(c, g):
        slot = lax.rem(c, RING)
        return pltpu.make_async_remote_copy(
            src_ref=own.at[slot, g], dst_ref=arrived.at[c, g + 1], send_sem=up_send.at[slot, g - 1],
            recv_sem=up_recv.at[c, g - 1], device_id={"lev": z + 1}, device_id_type=pl.DeviceIdType.MESH)

    def send_box(c, step):
        slot = lax.rem(c, 2)
        other = lax.rem(me + step, ma_size)
        return pltpu.make_async_remote_copy(
            src_ref=outbox.at[slot, other], dst_ref=inbox.at[c, me], send_sem=box_send.at[slot, step - 1],
            recv_sem=box_recv.at[c, step - 1], device_id={"ma": other}, device_id_type=pl.DeviceIdType.MESH)

    def recv_box(c, step):
        other = lax.rem(me + ma_size - step, ma_size)
        return pltpu.make_async_remote_copy(
            src_ref=outbox.at[0, me], dst_ref=inbox.at[c, other], send_sem=box_send.at[0, step - 1],
            recv_sem=box_recv.at[c, step - 1], device_id={"ma": other}, device_id_type=pl.DeviceIdType.MESH)

    def wait_sent(c):
        for g in range(top):
            @pl.when(g < z)
            def _():
                send_down(c, g).wait_send()
        for g in range(1, lev_size):
            @pl.when(g > z)
            def _():
                send_up(c, g).wait_send()

    def partial_sums(c):
        slot = lax.rem(c, 2)
        ring = lax.rem(c, RING)

        place = z * width_n + lax.broadcasted_iota(jnp.int32, (2 * level_count, width_n), 1)
        place = place.astype(f32)

        @pl.when(c >= 2)
        def _():
            store_fresh(c - 2).wait()

        def one(s, carry):
            offset = place - waves[0, me * slots + c * BATCH + s]
            value = decays[:, 0:1] * states[slot, s].reshape(2 * level_count, width_n) + amplitude[:, 0:width_n] * noises[
                slot, s].reshape(2 * level_count, width_n).astype(f32)
            value = jnp.where(offset >= 0, value, 0.0)
            fresh[slot, s] = value.reshape(2, level_count, width_n)
            odd = (offset[0:2 * levels].astype(jnp.int32) & 1) == 1
            parts = []
            for g in range(lev_size):
                even = jnp.concatenate([value[g * levels:(g + 1) * levels], value[
                    level_count + g * levels:level_count + (g + 1) * levels]], axis=0)
                parts += [even, jnp.where(odd, -even, even)]
            coef = jnp.concatenate(parts, axis=0).astype(bf16)
            product = jnp.dot(coef, weights[slot, s], preferred_element_type=f32)
            product = product.reshape(lev_size, 4 * levels, half)
            for g in range(lev_size):
                own[ring, g, pl.ds(pl.multiple_of(s * 4 * levels, 16), 4 * levels), :] = product[g].astype(bf16)
            return carry

        lax.fori_loop(0, BATCH, one, 0, unroll=4)
        store_fresh(c).start()

    def add(ring, g, value):
        own[ring, g] = (own[ring, g].astype(f32) + value.astype(f32)).astype(bf16)

    def pass_down(c):
        ring = lax.rem(c, RING)
        for g in range(top):
            @pl.when(g < z)
            def _():
                send_down(c, g).wait_recv()
                add(ring, g, arrived[c, g])
                send_down(c, g).start()

    def pass_up(c):
        ring = lax.rem(c, RING)
        for g in range(top, 0, -1):
            @pl.when(g > z)
            def _():
                send_up(c, g).wait_recv()
                add(ring, g, arrived[c, g + 1])
                send_up(c, g).start()

    def gather(c):
        total[...] = own[lax.rem(c, RING), z].astype(f32)

        @pl.when(z < top)
        def _():
            send_down(c, z).wait_recv()
            total[...] += arrived[c, z].astype(f32)

        @pl.when(z > 0)
        def _():
            send_up(c, z).wait_recv()
            total[...] += arrived[c, z + 1].astype(f32)

    def exchange(c):
        slot = lax.rem(c, 2)

        @pl.when(c >= 2)
        def _():
            for step in range(1, ma_size):
                send_box(c - 2, step).wait_send()

        parts = total[...].reshape(BATCH, 2, 2 * levels, half)
        flat = jnp.concatenate([parts[:, 0].reshape(-1, half), parts[:, 1].reshape(-1, half)], axis=1).astype(bf16)
        for first in range(0, ma_size * columns, 1024):
            rows_of = jnp.dot(flat, pick[:, first:first + 1024], preferred_element_type=f32)
            for t in range(1024 // LANES):
                gathered[first // LANES + t] = rows_of[:, t * LANES:(t + 1) * LANES]
        for step in range(ma_size):
            other = lax.rem(me + step, ma_size)
            tile = other * (columns // LANES)

            def put(lanes, value):
                if step:
                    outbox[slot, other, :, lanes] = value.astype(bf16)
                else:
                    inbox[c, me, :, lanes] = value.astype(bf16)

            for l in range(levels):
                for t in range(whole // LANES):
                    put(pl.ds(l * whole + t * LANES, LANES), gathered[tile + t, pl.ds(l, 2 * BATCH, stride=levels), :])
            if rest:
                each = LANES // pad
                lane = lax.broadcasted_iota(jnp.int32, (2 * BATCH, LANES), 1) // pad
                for first in range(0, levels, each):
                    mixed = None
                    for l in range(first, min(first + each, levels)):
                        value = gathered[tile + whole // LANES, pl.ds(l, 2 * BATCH, stride=levels), :]
                        mixed = value if mixed is None else jnp.where(lane == l - first, value, mixed)
                    put(pl.ds(levels * whole + first * pad, LANES), mixed)
            if step:
                send_box(c, step).start()

    depth = ma_size * 2 * BATCH
    held = basis.shape[0]

    def waves_of(c):
        row = lax.broadcasted_iota(jnp.int32, (2 * BATCH, LANES), 0) // 2

        def one(n, carry):
            first = lax.rem(n, ma_size) * slots + (c - (pair - 1) + n // ma_size) * BATCH
            value = jnp.zeros((2 * BATCH, LANES), f32)
            for s in range(BATCH):
                value = jnp.where(row == s, waves[0, first + s], value)
            wave_rows[pl.ds(pl.multiple_of(n * 2 * BATCH, 2 * BATCH), 2 * BATCH), :] = value
            return carry

        lax.fori_loop(0, pair * ma_size, one, 0)
        wave = wave_rows[...]
        lane = lax.broadcasted_iota(jnp.int32, wave.shape, 1).astype(f32)
        part = (lax.broadcasted_iota(jnp.int32, wave.shape, 0) & 1).astype(f32)
        factor = jnp.where(wave == 0.0, 1.0, 2.0)
        fine = wave * lane
        fine_cos, fine_sin = table(fine, width), table(fine - width // 4, width)
        rough = wave * (lane * LANES) + part * (width // 4)
        coarse_cos, coarse_sin = factor * table(rough, width), factor * table(rough - width // 4, width)
        slot = lax.rem(c // pair, held)
        for a in range(width // LANES):
            value = coarse_cos[:, a:a + 1] * fine_cos - coarse_sin[:, a:a + 1] * fine_sin
            basis[slot, :, a * LANES:(a + 1) * LANES] = value.astype(bf16)

    def turn(c):
        for k in range(pair):
            for step in range(1, ma_size):
                recv_box(c - (pair - 1) + k, step).wait_recv()
        spread = inbox[pl.ds(c - (pair - 1), pair)]
        turned[...] = jnp.transpose(spread.reshape(pair * depth, spread.shape[-1]))

    def transform(c):
        turn(c)

        def one(n, carry):
            lanes = pl.ds(pl.multiple_of(n * 256, 256), 256)
            acc[:, lanes] += jnp.dot(turned[...], basis[lax.rem(c // pair, held), :, lanes], preferred_element_type=f32)
            return carry

        lax.fori_loop(0, width // 256, one, 0)

    def finish(c):
        turn(c)
        for n in range(width // 256):
            lanes = pl.ds(n * 256, 256)
            value = (acc[:, lanes] + jnp.dot(
                turned[...], basis[(c // pair) % held, :, lanes], preferred_element_type=f32)).astype(bf16)
            for l in range(levels):
                if whole:
                    pattern[l, 0:whole, lanes] = value[l * whole:(l + 1) * whole]
                if rest:
                    first = levels * whole + l * pad
                    pattern[l, whole:rows, lanes] = value[first:first + rest]

    barrier = pltpu.get_barrier_semaphore()
    for step in range(1, ma_size):
        pl.semaphore_signal(barrier, inc=1, device_id={"ma": lax.rem(me + step, ma_size)},
                            device_id_type=pl.DeviceIdType.MESH)

    @pl.when(z > 0)
    def _():
        pl.semaphore_signal(barrier, inc=1, device_id={"lev": z - 1}, device_id_type=pl.DeviceIdType.MESH)

    @pl.when(z < top)
    def _():
        pl.semaphore_signal(barrier, inc=1, device_id={"lev": z + 1}, device_id_type=pl.DeviceIdType.MESH)

    small = [pltpu.make_async_copy(src, dst, small_sem.at[n]) for n, (src, dst) in enumerate((
        (small_in.at[:, pl.ds(0, waves.shape[1])], waves),
        (small_in.at[:, pl.ds(waves.shape[1], amplitude.shape[1])], amplitude),
        (small_in.at[:, pl.ds(waves.shape[1] + amplitude.shape[1], LANES)], decay), (source_in, source)))]
    for copy in small:
        copy.start()
    fetch(0, "start")
    for copy in small:
        copy.wait()
    level = lax.rem(lax.broadcasted_iota(jnp.int32, decays.shape, 0), level_count)
    rate = jnp.zeros(decays.shape, f32)
    for l in range(level_count):
        rate = jnp.where(level == l, decay[0, l], rate)
    decays[...] = rate
    fetch(0, "wait")
    partial_sums(0)
    inner = (z > 0) & (z < top)

    @pl.when(inner)
    def _():
        pl.semaphore_wait(barrier, ma_size + 1)

    @pl.when(jnp.logical_not(inner))
    def _():
        pl.semaphore_wait(barrier, ma_size)

    def step(i, carry):
        @pl.when(i < chunks)
        def _():
            @pl.when(i + 1 < chunks)
            def _():
                fetch(i + 1, "start")

            @pl.when(i > 0)
            def _():
                fetch(i, "wait")

                @pl.when(i >= RING)
                def _():
                    wait_sent(i - RING)

                partial_sums(i)

            @pl.when(z == top)
            def _():
                for g in range(top - 1):
                    send_down(i, g).start()

                @pl.when(i > 0)
                def _():
                    send_down(i - 1, top - 1).start()

                @pl.when(i == chunks - 1)
                def _():
                    send_down(i, top - 1).start()

            @pl.when(z == 0)
            def _():
                for g in range(top, 1, -1):
                    send_up(i, g).start()

                @pl.when(i > 0)
                def _():
                    send_up(i - 1, 1).start()

                @pl.when(i == chunks - 1)
                def _():
                    send_up(i, 1).start()

        @pl.when(i == 0)
        def _():
            acc[...] = jnp.zeros_like(acc)
            row = lax.broadcasted_iota(jnp.int32, (2 * half, columns), 0)
            for j in range(ma_size):
                pick[:, j * columns:(j + 1) * columns] = jnp.where(row == source[:, j * columns:(j + 1) * columns], 1.0, 0.0).astype(bf16)

        def stage(lag, active, work):
            c = i - lag

            @pl.when((c >= 0) & (c < chunks) & active)
            def _():
                work(c)

        early = far - 2
        stage(early, lax.rem(i - early + pair, pair) == pair - 1, waves_of)
        stage(LAG + top - z, z < top, pass_down)
        stage(LAG + z, z > 0, pass_up)
        stage(far, z >= 0, gather)
        stage(far, z >= 0, exchange)
        stage(far + 1, (lax.rem(i - far - 1 + pair, pair) == pair - 1) & (i - far - 1 < chunks - 1), transform)
        return carry

    lax.fori_loop(0, chunks + LAG + top, step, 0)
    finish(chunks - 1)
    for c in range(max(0, chunks - 2), chunks):
        store_fresh(c).wait()
    for c in range(max(0, chunks - RING), chunks):
        wait_sent(c)
    for c in range(max(0, chunks - 2), chunks):
        for s in range(1, ma_size):
            send_box(c, s).wait_send()


def deliver(made_state, made_pattern, new_state, pattern, sems):
    piece = made_state.shape[0] // PIECES
    copies = [pltpu.make_async_copy(made_state.at[pl.ds(n * piece, piece)], new_state.at[pl.ds(n * piece, piece)],
                                    sems.at[n]) for n in range(PIECES)]
    copies.append(pltpu.make_async_copy(made_pattern, pattern, sems.at[PIECES]))
    for copy in copies:
        copy.start()
    for copy in copies:
        copy.wait()


def make_body(ma_size, lev_size):
    def body(spectral_state, forcing_noise, decay_rate, amplitude, legendre, wave_of_slot, lat_of_row):
        slot_count, _, level_count, width_n = spectral_state.shape
        levels = level_count // lev_size
        half = legendre.shape[2]
        lat_count = lat_of_row.shape[0]
        width = 2 * lat_count
        rows = lat_count // ma_size
        chunks = slot_count // BATCH
        whole, rest, pad = row_plan(rows)
        source = jnp.where(lat_of_row < half, lat_of_row, half + lat_count - 1 - lat_of_row)
        source = source.astype(jnp.int32).reshape(ma_size, rows)
        if rest:
            tail = jnp.pad(source[:, whole:], ((0, 0), (0, pad - rest)), constant_values=-1)
            source = jnp.concatenate([source[:, :whole], jnp.tile(tail, (1, LANES // pad))], axis=1)
        columns = source.shape[1]
        depth = ma_size * 2 * BATCH
        pair = max(1, 256 // depth)
        spread = levels * (whole + pad)
        tall = BATCH * 4 * levels
        dims = (ma_size, lev_size, chunks, levels, rows, half, width, pair)
        any_space = pl.BlockSpec(memory_space=pl.ANY)
        vmem = pl.BlockSpec(memory_space=pltpu.VMEM)
        dma = pltpu.SemaphoreType.DMA
        source = source.reshape(1, -1)
        small = jnp.concatenate([
            wave_of_slot.astype(f32), jnp.pad(amplitude, (0, -width_n % LANES)), jnp.pad(decay_rate, (0, LANES - level_count))])
        ring = ring_of(lev_size)
        arrays = [
            ((1, -(-width_n // LANES) * LANES), f32), (source.shape, jnp.int32),
            ((2, BATCH, 2, level_count, width_n), f32),
            ((2, BATCH, 2, level_count, width_n), bf16),
            ((2, BATCH, 2, level_count, width_n), f32),
            ((2, BATCH, width_n, half), bf16),
            ((2 * level_count, LANES), f32),
            ((pair * depth, LANES), f32),
            ((ring, lev_size, tall, half), bf16),
            ((chunks, lev_size + 1, tall, half), bf16),
            ((tall, half), f32),
            ((2 * half, ma_size * columns), bf16),
            ((ma_size * columns // LANES, BATCH * 2 * levels, LANES), f32),
            ((2, ma_size, 2 * BATCH, spread), bf16),
            ((chunks, ma_size, 2 * BATCH, spread), bf16),
            ((spread, pair * depth), bf16),
            ((3 // pair + 1, pair * depth, width), bf16),
            ((spread, width), f32),
        ]
        scratch = [pltpu.VMEM(shape, kind) for shape, kind in arrays]
        bytes_held = sum(math.prod(shape[:-1]) * -(-shape[-1] // LANES) * LANES * jnp.dtype(kind).itemsize
                         for shape, kind in arrays)
        smem = pltpu.SMEM
        made = pl.pallas_call(
            functools.partial(kernel, dims),
            out_shape=(jax.ShapeDtypeStruct(spectral_state.shape, f32),
                       jax.ShapeDtypeStruct((levels, rows, width), bf16)),
            in_specs=[any_space, any_space, any_space] + [any_space] * 2,
            out_specs=(any_space, vmem),
            scratch_shapes=[
                smem((1, LANES), f32), scratch[0], smem((1, wave_of_slot.shape[0]), f32), *scratch[1:],
                dma((4,)),
                dma((2,)), dma((2,)), dma((2,)), dma((2,)),
                dma((ring, lev_size - 1)), dma((ring, lev_size - 1)),
                dma((chunks, lev_size - 1)), dma((chunks, lev_size - 1)),
                dma((2, ma_size - 1)), dma((chunks, ma_size - 1)),
            ],
            compiler_params=pltpu.CompilerParams(
                collective_id=0, has_side_effects=True, vmem_limit_bytes=min(bytes_held + SPARE, 67043328)),
        )(spectral_state, forcing_noise, legendre, small.reshape(1, -1), source)
        return pl.pallas_call(
            deliver,
            out_shape=(jax.ShapeDtypeStruct(spectral_state.shape, f32),
                       jax.ShapeDtypeStruct((levels, rows, width), bf16)),
            in_specs=[vmem, vmem],
            out_specs=(any_space, any_space),
            scratch_shapes=[dma((PIECES + 1,))],
            compiler_params=pltpu.CompilerParams(vmem_limit_bytes=16 * 1024 * 1024),
        )(*made)

    return body


def solution(mesh):
    return jax.shard_map(
        make_body(mesh.shape["ma"], mesh.shape["lev"]),
        mesh=mesh,
        in_specs=(
            P("ma", None, None, "lev"),
            P("ma", None, None, "lev"),
            P(),
            P("lev"),
            P("ma", "lev", None),
            P(),
            P(),
        ),
        out_specs=(P("ma", None, None, "lev"), P("lev", "ma", None)),
        check_vma=False,
    )
```
